512 devices in a mesh: head: 2 (over core), ctx: 256 (over z, y, x).
Axes of the slice: x: 4, y: 8, z: 8, core: 2. Of those that a mesh axis runs over, the one named last changes fastest.
Arguments:
- queries: bfloat16 [65536, 4096], P(('ctx', 'head')), may hold values from -6 to 6
- keys: bfloat16 [65536, 512], P(('ctx', 'head')), may hold values from -6 to 6
- values: bfloat16 [65536, 512], P(('ctx', 'head')), may hold values from -6 to 6
- attn_out: bfloat16 [65536, 4096], P(('ctx', 'head')), may hold values from -6 to 6
- output_gradient: bfloat16 [65536, 4096], P(('ctx', 'head')), may hold values from -6 to 6
- doc_lengths: int32 [512], replicated, may hold values from 1 to 257, 65536 in all
Outputs:
- query_grad: bfloat16 [65536, 4096], P(('ctx', 'head'))
- key_gradient: bfloat16 [65536, 512], P(('ctx', 'head'))
- value_gradient: bfloat16 [65536, 512], P(('ctx', 'head'))
The draws below stay inside these ranges and needn't reach their ends.
Inputs may be any that keep to these rules, and one draw needn't show every extreme that they name: `doc_lengths`: documents fill the 65536 tokens in order; one document has exactly 257 tokens.
All inputs are finite; a program needn't handle non-finite values.
Results may differ from the reference program's by a relative error of at most 0.0054.
Values may be sent and summed in bfloat16 or wider, within the bound.
No kernel may reach another device: no remote copies, remote signals or barrier semaphores. Data moves between devices by JAX's collectives and lax.ppermute only.
A program may use at most 64 MiB of HBM per device.

```python
import math
import jax
import jax.numpy as jnp
import numpy as np
from jax import lax

QUERY_HEAD_COUNT = 32
KEY_VALUE_HEADS = 4
HEAD_SIZE = 128
REACH = 1
CONTEXT_TOKENS = 256
PACKED_TOKENS = 65536
MOST = 257
NDOC = 512
N_CTX = 256


def draw_keys(key, part):
    drawn_result = jnp.clip(jax.random.normal(jax.random.fold_in(key, 3), (PACKED_TOKENS, KEY_VALUE_HEADS * HEAD_SIZE), jnp.float32), -6.0, 6.0)
    return drawn_result.astype(jnp.bfloat16)


def draw_queries(key, part):
    drawn_result = jnp.clip(jax.random.normal(jax.random.fold_in(key, 4), (PACKED_TOKENS, QUERY_HEAD_COUNT * HEAD_SIZE), jnp.float32), -6.0, 6.0)
    return drawn_result.astype(jnp.bfloat16)


def block_levels(own_key, dims, cuts, smallest, high):
    gain = 1.0
    for position, parts in cuts:
        draws = jax.random.uniform(jax.random.fold_in(jax.random.fold_in(own_key, 6), position), (parts,), jnp.float32, smallest / len(cuts), high / len(cuts))
        gain = gain * jnp.repeat(jnp.exp(draws), dims[position] // parts).reshape((-1,) + (1,) * (len(dims) - 1 - position))
    return gain


def length_profile(number_of, total, bound, skew):
    loads = [(1 << 20) // math.isqrt(rank ** skew) + 1 for rank in range(2, number_of + 1)]
    spare, counts = total - bound - (number_of - 1), [1] * (number_of - 1)
    while spare > 0:
        movable = [i for i in range(number_of - 1) if counts[i] < bound]
        pool, left = sum([loads[i] for i in movable]), spare
        for i in movable:
            extra = min(bound - counts[i], max(1, left * loads[i] // pool), spare)
            counts[i] = counts[i] + extra
            spare = spare - extra
    return np.array([bound] + counts)


def ragged_sizes(rng, amount, total, bound, slope):
    if amount == 2:
        one = jax.random.randint(rng, (), max(1, total - bound), min(bound, total - 1) + 1)
        return jnp.stack([one, total - one])
    lengths = jnp.asarray(length_profile(amount, total, bound, slope), jnp.int32)
    couples = (amount - 1) // 2
    giver, taker = lengths[1:1 + 2 * couples:2], lengths[2:2 + 2 * couples:2]
    margin = jnp.minimum(giver - 1, bound - taker)
    moved = jax.random.randint(jax.random.fold_in(rng, 1), (couples,), 0, 1 << 20) % (margin + 1)
    lengths = lengths.at[1:1 + 2 * couples:2].set(giver - moved).at[2:2 + 2 * couples:2].set(taker + moved)
    return lengths[jax.random.permutation(jax.random.fold_in(rng, 2), amount)]


def normal_values(rng, extent, deviation, bound, shards=(), kind=jnp.bfloat16):
    drawn = deviation * jax.random.normal(rng, extent, jnp.float32)
    if shards:
        drawn = drawn * block_levels(rng, extent, shards, -0.22, 0.18)
    return jnp.clip(drawn, -bound, bound).astype(kind)


def setup_inputs(seed: int = 0) -> dict:
    key_of = jax.random.split(jax.random.key(seed), 7)
    queries = draw_queries(jax.random.fold_in(key_of[6], 71), 0)
    keys = draw_keys(jax.random.fold_in(key_of[6], 71), 0)
    values = normal_values(key_of[2], (PACKED_TOKENS, KEY_VALUE_HEADS * HEAD_SIZE), 1.0, 6.0, ((0, 512),))
    attn_out = normal_values(key_of[3], (PACKED_TOKENS, QUERY_HEAD_COUNT * HEAD_SIZE), 1.0, 6.0, ((0, 512),))
    output_gradient = normal_values(key_of[4], (PACKED_TOKENS, QUERY_HEAD_COUNT * HEAD_SIZE), 1.0, 6.0, ((0, 512),))
    doc_lengths = ragged_sizes(key_of[5], NDOC, PACKED_TOKENS, MOST, 2).astype(jnp.int32)
    return dict(queries=queries, keys=keys, values=values, attn_out=attn_out, output_gradient=output_gradient, doc_lengths=doc_lengths)


fill_value = -1e30


def segment_ids(doc_lengths, positions):
    ends = jnp.cumsum(doc_lengths).astype(jnp.int32)
    return jnp.sum((ends[None, :] <= positions[:, None]).astype(jnp.int32), axis=1, dtype=jnp.int32)


def round_low(array):
    return lax.optimization_barrier(array.astype(jnp.bfloat16)).astype(jnp.float32)


def reference(queries, keys, values, attn_out, output_gradient, doc_lengths):
    group_width = QUERY_HEAD_COUNT // KEY_VALUE_HEADS
    score_scale = HEAD_SIZE ** -0.5
    width = (REACH + 1) * CONTEXT_TOKENS
    margin_amount = REACH * CONTEXT_TOKENS
    delta_value = jnp.sum((output_gradient.astype(jnp.float32) * attn_out.astype(jnp.float32)).reshape(PACKED_TOKENS, QUERY_HEAD_COUNT, HEAD_SIZE), axis=2).astype(jnp.bfloat16)
    seg_all = segment_ids(doc_lengths, jnp.arange(PACKED_TOKENS, dtype=jnp.int32))
    seg_pad = jnp.concatenate([jnp.full((margin_amount,), -1, jnp.int32), seg_all])
    pos_pad = jnp.arange(PACKED_TOKENS + margin_amount, dtype=jnp.int32) - margin_amount
    padded_keys = jnp.pad(keys.reshape(PACKED_TOKENS, KEY_VALUE_HEADS, HEAD_SIZE), ((margin_amount, 0), (0, 0), (0, 0)))
    padded_values = jnp.pad(values.reshape(PACKED_TOKENS, KEY_VALUE_HEADS, HEAD_SIZE), ((margin_amount, 0), (0, 0), (0, 0)))

    def block(carry, block_index):
        key_running_sum, value_running_sum = carry
        start_index = (block_index * CONTEXT_TOKENS).astype(jnp.int32)
        query_row_block = lax.dynamic_slice_in_dim(queries, start_index, CONTEXT_TOKENS, 0).reshape(CONTEXT_TOKENS, KEY_VALUE_HEADS, group_width, HEAD_SIZE).astype(jnp.float32)
        gradient_row_block = lax.dynamic_slice_in_dim(output_gradient, start_index, CONTEXT_TOKENS, 0).reshape(CONTEXT_TOKENS, KEY_VALUE_HEADS, group_width, HEAD_SIZE).astype(jnp.float32)
        row_delta_values = lax.dynamic_slice_in_dim(delta_value, start_index, CONTEXT_TOKENS, 0).reshape(CONTEXT_TOKENS, KEY_VALUE_HEADS, group_width).astype(jnp.float32)
        row_delta_values = jnp.transpose(row_delta_values, (1, 2, 0))
        key_rows = lax.dynamic_slice_in_dim(padded_keys, start_index, width, 0).astype(jnp.float32)
        value_rows = lax.dynamic_slice_in_dim(padded_values, start_index, width, 0).astype(jnp.float32)
        seg_query = lax.dynamic_slice_in_dim(seg_all, start_index, CONTEXT_TOKENS, 0)
        seg_key = lax.dynamic_slice_in_dim(seg_pad, start_index, width, 0)
        pos_query = start_index + jnp.arange(CONTEXT_TOKENS, dtype=jnp.int32)
        pos_key = lax.dynamic_slice_in_dim(pos_pad, start_index, width, 0)
        allowed = (seg_query[:, None] == seg_key[None, :]) & (pos_key[None, :] <= pos_query[:, None])
        scores = jnp.einsum('tkgd,ukd->kgtu', query_row_block, key_rows, precision=lax.Precision.HIGHEST) * score_scale
        masked = jnp.where(allowed, scores, fill_value)
        row_max = jnp.max(masked, axis=-1)
        row_sum = jnp.sum(jnp.where(allowed, jnp.exp(masked - row_max[..., None]), 0.0), axis=-1)
        lse = row_max + jnp.log(row_sum)
        probs = jnp.where(allowed, jnp.exp(jnp.where(allowed, scores - lse[..., None], fill_value)), 0.0)
        probs_low = round_low(probs)
        prob_grad = jnp.einsum('tkgd,ukd->kgtu', gradient_row_block, value_rows, precision=lax.Precision.HIGHEST)
        score_grad = round_low(probs * (prob_grad - row_delta_values[..., None]))
        query_part = jnp.einsum('kgtu,ukd->tkgd', score_grad, key_rows, precision=lax.Precision.HIGHEST) * score_scale
        key_part = jnp.einsum('kgtu,tkgd->ukd', score_grad, query_row_block, precision=lax.Precision.HIGHEST) * score_scale
        value_part = jnp.einsum('kgtu,tkgd->ukd', probs_low, gradient_row_block, precision=lax.Precision.HIGHEST)
        key_running_sum = lax.dynamic_update_slice_in_dim(key_running_sum, lax.dynamic_slice_in_dim(key_running_sum, start_index, width, 0) + key_part, start_index, 0)
        value_running_sum = lax.dynamic_update_slice_in_dim(value_running_sum, lax.dynamic_slice_in_dim(value_running_sum, start_index, width, 0) + value_part, start_index, 0)
        return (key_running_sum, value_running_sum), query_part.reshape(CONTEXT_TOKENS, QUERY_HEAD_COUNT * HEAD_SIZE).astype(jnp.bfloat16)

    zero_running_sum = jnp.zeros((PACKED_TOKENS + margin_amount, KEY_VALUE_HEADS, HEAD_SIZE), jnp.float32)
    (key_running_sum, value_running_sum), query_blocks = lax.scan(block, (zero_running_sum, zero_running_sum), jnp.arange(N_CTX, dtype=jnp.int32))
    query_grad = query_blocks.reshape(PACKED_TOKENS, QUERY_HEAD_COUNT * HEAD_SIZE)
    key_gradient = key_running_sum[margin_amount:].reshape(PACKED_TOKENS, KEY_VALUE_HEADS * HEAD_SIZE).astype(jnp.bfloat16)
    value_gradient = value_running_sum[margin_amount:].reshape(PACKED_TOKENS, KEY_VALUE_HEADS * HEAD_SIZE).astype(jnp.bfloat16)
    return (query_grad, key_gradient, value_gradient)
```

```python
import jax
import jax.numpy as jnp
from jax import lax
from jax.experimental import pallas as pl
from jax.experimental.pallas import tpu as pltpu
from jax.sharding import PartitionSpec as P

HEADS = 32
GROUPS = 4
PER_GROUP = HEADS // GROUPS
PAIRS = PER_GROUP // 2
DIM = 128
ROWS = 128
WIDE = GROUPS * DIM
FULL = HEADS * DIM
GROUP_COLS = PER_GROUP * DIM
SCALE = DIM ** (-0.5)
LOG2E = 1.4426950408889634
TO_BITS = SCALE * LOG2E
FILL = -1e30
VMEM = pltpu.VMEM
F32 = jnp.float32
BF16 = jnp.bfloat16
NT = (((1,), (1,)), ((), ()))
NN = (((1,), (0,)), ((), ()))


def dot(a, b, dims):
    return lax.dot_general(a, b, dims, preferred_element_type=F32)


def span(start, size):
    return pl.ds(pl.multiple_of(start, DIM), size)


def stacked(ref, first, count):
    return jnp.concatenate([ref[:, span(first + i * DIM, DIM)] for i in range(count)], axis=0)


def pack_kernel(k_ref, v_ref, out_ref, sems):
    first = pltpu.make_async_copy(k_ref, out_ref.at[:, pl.ds(0, WIDE)], sems.at[0])
    second = pltpu.make_async_copy(v_ref, out_ref.at[:, pl.ds(WIDE, WIDE)], sems.at[1])
    first.start()
    second.start()
    first.wait()
    second.wait()


def local_kernel(
    pos_ref, len_hbm, q_hbm, g_hbm, o_hbm, kv_ref,
    q_ref, g_ref, start_ref, delta_ref, max_ref, sum_ref,
    len_ref, o_ref, sems, len_sem,
):
    def copies(g):
        cols = span(g * GROUP_COLS, GROUP_COLS)
        return [
            pltpu.make_async_copy(src.at[:, cols], dst.at[:, cols], sems.at[i, g])
            for i, (src, dst) in enumerate(((q_hbm, q_ref), (g_hbm, g_ref), (o_hbm, o_ref)))
        ]

    len_copy = pltpu.make_async_copy(len_hbm, len_ref, len_sem)
    len_copy.start()
    for g in range(GROUPS):
        for copy in copies(g):
            copy.start()
    len_copy.wait()
    base = pos_ref[0]
    count = len_ref.shape[1]
    lengths = len_ref[...]
    high = lax.shift_right_logical(lengths, 4)
    low = lengths - high * 16
    both = jnp.concatenate(
        [jnp.broadcast_to(high, (8, count)), jnp.broadcast_to(low, (8, count))], axis=0
    ).astype(F32).astype(BF16)
    row = lax.broadcasted_iota(jnp.int32, (count, count), 0)
    col = lax.broadcasted_iota(jnp.int32, (count, count), 1)
    lower = jnp.where(col <= row, 1.0, 0.0).astype(BF16)
    sums = dot(lower, both, NT)
    ends = sums[:, 0:1] * 16.0 + sums[:, 8:9]
    tokens = (base + lax.broadcasted_iota(jnp.int32, (count, ROWS), 1)).astype(F32)
    starts = jnp.max(jnp.where(ends <= tokens, ends, 0.0), axis=0, keepdims=True)
    starts = starts - base.astype(F32)
    starts = jnp.concatenate([starts, starts], axis=1)
    start_ref[...] = jnp.broadcast_to(starts, (8, 2 * ROWS))
    key_at = lax.broadcasted_iota(jnp.int32, (ROWS, 2 * ROWS), 0)
    query_at = lax.broadcasted_iota(jnp.int32, (ROWS, 2 * ROWS), 1) & (ROWS - 1)
    seen = (key_at <= query_at) & (key_at.astype(F32) >= starts)

    def group(g, carry):
        for copy in copies(g):
            copy.wait()
        keys = kv_ref[:, span(g * DIM, DIM)]
        for p in range(PAIRS):
            pair = g * PAIRS + p
            first = pair * 2 * DIM
            deltas = []
            for h in range(2):
                cols = span(first + h * DIM, DIM)
                prod = g_ref[:, cols].astype(F32) * o_ref[:, cols].astype(F32)
                deltas.append(jnp.sum(prod.T, axis=0, keepdims=True))
            delta = jnp.concatenate(deltas, axis=1)
            delta_ref[pl.ds(pair, 1), :] = delta.astype(BF16).astype(F32)
            scores = dot(keys, stacked(q_ref, first, 2), NT)
            scores = jnp.where(seen, scores, FILL)
            top = jnp.max(scores, axis=0, keepdims=True)
            max_ref[pl.ds(pair, 1), :] = top
            sum_ref[pl.ds(pair, 1), :] = jnp.sum(
                jnp.exp2(scores * TO_BITS - top * TO_BITS), axis=0, keepdims=True
            )
        return carry

    lax.fori_loop(0, GROUPS, group, 0)


def far_kernel(
    start_ref, delta_ref, max_ref, sum_ref, q_ref, g_ref, kv2_ref, kv1_ref,
    out_ref, p1_ref, ds2_ref, bits_ref,
    bias_ref, p2_ref,
):
    key_at = lax.broadcasted_iota(jnp.int32, (2 * ROWS, ROWS), 0).astype(F32) - 2.0 * ROWS
    bias_ref[...] = jnp.where(key_at >= start_ref[0:1, :ROWS], 0.0, FILL)

    def group(g, carry):
        gcols = span(g * DIM, DIM)
        keys2 = kv2_ref[:, gcols]
        keys1 = kv1_ref[:, gcols]
        values2 = kv2_ref[:, span(WIDE + g * DIM, DIM)]
        bias2 = jnp.concatenate([bias_ref[:ROWS, :]] * 2, axis=1)
        bias1 = jnp.concatenate([bias_ref[ROWS:, :]] * 2, axis=1)
        for p in range(PAIRS):
            pair = g * PAIRS + p
            first = pair * 2 * DIM
            query = stacked(q_ref, first, 2)
            scores2 = dot(keys2, query, NT) + bias2
            scores1 = dot(keys1, query, NT) + bias1
            own_max = max_ref[pl.ds(pair, 1), :]
            top = jnp.maximum(
                jnp.max(jnp.maximum(scores2, scores1), axis=0, keepdims=True), own_max
            )
            bits = top * TO_BITS
            exps2 = jnp.exp2(scores2 * TO_BITS - bits)
            exps1 = jnp.exp2(scores1 * TO_BITS - bits)
            denom = jnp.sum(exps2 + exps1, axis=0, keepdims=True) + sum_ref[
                pl.ds(pair, 1), :
            ] * jnp.exp2(own_max * TO_BITS - bits)
            bits_ref[pl.ds(pair, 1), :] = bits + jnp.log2(denom)
            inverse = 1.0 / denom
            probs2 = exps2 * inverse
            cols = span(first, 2 * DIM)
            p1_ref[:, cols] = (exps1 * inverse).astype(BF16)
            p2_ref[:, pl.ds(p * 2 * DIM, 2 * DIM)] = probs2.astype(BF16)
            grads = dot(values2, stacked(g_ref, first, 2), NT)
            ds2_ref[:, cols] = (probs2 * (grads - delta_ref[pl.ds(pair, 1), :])).astype(BF16)
        head0 = g * GROUP_COLS
        dk = dot(ds2_ref[:, span(head0, GROUP_COLS)], stacked(q_ref, head0, PER_GROUP), NN)
        dv = dot(p2_ref[...], stacked(g_ref, head0, PER_GROUP), NN)
        out_ref[:, gcols] = (dk * SCALE).astype(BF16)
        out_ref[:, span(WIDE + g * DIM, DIM)] = dv.astype(BF16)
        return carry

    lax.fori_loop(0, GROUPS, group, 0)


def near_kernel(delta_ref, p1_ref, q_ref, g_ref, kv1_ref, after_ref, out_ref, ds1_ref):
    def group(g, carry):
        gcols = span(g * DIM, DIM)
        values = kv1_ref[:, span(WIDE + g * DIM, DIM)]
        for p in range(PAIRS):
            pair = g * PAIRS + p
            first = pair * 2 * DIM
            cols = span(first, 2 * DIM)
            grads = dot(values, stacked(g_ref, first, 2), NT)
            probs = p1_ref[:, cols].astype(F32)
            ds1_ref[:, cols] = (probs * (grads - delta_ref[pl.ds(pair, 1), :])).astype(BF16)
        head0 = g * GROUP_COLS
        wide = span(head0, GROUP_COLS)
        dk = dot(ds1_ref[:, wide], stacked(q_ref, head0, PER_GROUP), NN)
        dv = dot(p1_ref[:, wide], stacked(g_ref, head0, PER_GROUP), NN)
        out_ref[:, gcols] = (dk * SCALE).astype(BF16)
        out_ref[:, span(WIDE + g * DIM, DIM)] = dv.astype(BF16)
        return carry

    lax.fori_loop(0, GROUPS, group, 0)


def own_kernel(
    start_ref, delta_ref, bits_ref, q_ref, g_ref, kv_ref, kv2_ref, kv1_ref, ds2_ref, ds1_ref, after_ref,
    dq_hbm, out_ref,
    ds_ref, p_ref, dq_ref, sems,
):
    key_at = lax.broadcasted_iota(jnp.int32, (ROWS, 2 * ROWS), 0)
    query_at = lax.broadcasted_iota(jnp.int32, (ROWS, 2 * ROWS), 1) & (ROWS - 1)
    seen = (key_at <= query_at) & (key_at.astype(F32) >= start_ref[0:1, :])

    def copy(g):
        cols = span(g * GROUP_COLS, GROUP_COLS)
        return pltpu.make_async_copy(dq_ref.at[:, cols], dq_hbm.at[:, cols], sems.at[g])

    def group(g, carry):
        gcols = span(g * DIM, DIM)
        vcols = span(WIDE + g * DIM, DIM)
        keys = kv_ref[:, gcols]
        values = kv_ref[:, vcols]
        turned = jnp.concatenate([kv2_ref[:, gcols].T, kv1_ref[:, gcols].T, keys.T], axis=1)
        for p in range(PAIRS):
            pair = g * PAIRS + p
            first = pair * 2 * DIM
            cols = span(first, 2 * DIM)
            here = pl.ds(p * 2 * DIM, 2 * DIM)
            scores = dot(keys, stacked(q_ref, first, 2), NT)
            probs = jnp.exp2(
                jnp.where(seen, scores * TO_BITS - bits_ref[pl.ds(pair, 1), :], FILL)
            )
            grads = dot(values, stacked(g_ref, first, 2), NT)
            low = (probs * (grads - delta_ref[pl.ds(pair, 1), :])).astype(BF16)
            ds_ref[:, here] = low
            p_ref[:, here] = probs.astype(BF16)
            score_grads = jnp.concatenate([ds2_ref[:, cols], ds1_ref[:, cols], low], axis=0)
            turned_grad = dot(turned, score_grads, NN) * SCALE
            for h in range(2):
                dq_ref[:, span(first + h * DIM, DIM)] = (
                    turned_grad[:, h * DIM:(h + 1) * DIM].T.astype(BF16)
                )
        copy(g).start()
        head0 = g * GROUP_COLS
        dk = dot(ds_ref[...], stacked(q_ref, head0, PER_GROUP), NN)
        dv = dot(p_ref[...], stacked(g_ref, head0, PER_GROUP), NN)
        out_ref[:, gcols] = dk * SCALE
        out_ref[:, vcols] = dv
        return carry

    lax.fori_loop(0, GROUPS, group, 0)
    for g in range(GROUPS):
        copy(g).wait()


def sum_kernel(own_ref, far_ref, near_ref, dk_ref, dv_ref):
    for part, ref in ((0, dk_ref), (1, dv_ref)):
        cols = pl.ds(part * WIDE, WIDE)
        total = own_ref[:, cols] + far_ref[:, cols].astype(F32) + near_ref[:, cols].astype(F32)
        ref[...] = total.astype(BF16)


def call(body, name, flops, ins, outs, scratch=()):
    spaces = {"s": pltpu.SMEM, "v": VMEM, "a": pl.ANY, "h": pltpu.HBM}
    return pl.pallas_call(
        body,
        name=name,
        in_specs=[pl.BlockSpec(memory_space=spaces[space]) for space in ins],
        out_specs=[pl.BlockSpec(memory_space=spaces[space]) for space, _, _ in outs],
        out_shape=[jax.ShapeDtypeStruct(shape, dtype) for _, shape, dtype in outs],
        scratch_shapes=list(scratch),
        cost_estimate=pl.CostEstimate(flops=flops, transcendentals=0, bytes_accessed=1 << 20),
        compiler_params=pltpu.CompilerParams(vmem_limit_bytes=12 << 20),
    )


def on_device(queries, keys, values, attn_out, output_gradient, doc_lengths):
    contexts = lax.axis_size("ctx")
    halves = lax.axis_size("head")
    blocks = contexts * halves
    count = doc_lengths.shape[0]

    def shifted(array, by):
        place = lambda i: (i % halves) * contexts + i // halves
        pairs = [(place(i), place(i + by)) for i in range(blocks) if 0 <= i + by < blocks]
        return lax.ppermute(array, ("head", "ctx"), pairs)

    keys, values, queries, attn_out, output_gradient, lengths = (
        pltpu.with_memory_space_constraint(array, pltpu.HBM)
        for array in (keys, values, queries, attn_out, output_gradient, doc_lengths.reshape(1, -1))
    )
    base = ((lax.axis_index("ctx") * halves + lax.axis_index("head")) * ROWS).reshape(1)
    stat = ("v", (HEADS // 2, 2 * ROWS), F32)
    rows = ("v", (8, 2 * ROWS), F32)
    both = ("v", (ROWS, 2 * WIDE), BF16)
    full = ("v", (ROWS, FULL), BF16)
    narrow = ("v", (ROWS, WIDE), BF16)
    dma = pltpu.SemaphoreType.DMA
    (kv,) = call(pack_kernel, "pack", 1 << 20, "hh", [both], [dma((2,))])(keys, values)
    kv2 = shifted(kv, 2)
    kv1 = shifted(kv, 1)
    q, g, start, delta, own_max, own_sum = call(
        local_kernel, "local", 1 << 30, "shhhhv", [full, full, rows, stat, stat, stat],
        [VMEM((1, count), jnp.int32), VMEM((ROWS, FULL), BF16), dma((3, GROUPS)), dma],
    )(base, lengths, queries, output_gradient, attn_out, kv)
    far, p1, ds2, bits = call(
        far_kernel, "far", 2 << 30, "v" * 8, [both, full, full, stat],
        [VMEM((2 * ROWS, ROWS), F32), VMEM((ROWS, GROUP_COLS), BF16)],
    )(start, delta, own_max, own_sum, q, g, kv2, kv1)
    back2 = shifted(far, -2)
    near, ds1 = call(near_kernel, "near", 1 << 30, "vvvvva", [both, full])(delta, p1, q, g, kv1, far)
    back1 = shifted(near, -1)
    query_grad, own = call(
        own_kernel, "own", 4 << 30, "v" * 10 + "a",
        [("h", (ROWS, FULL), BF16), ("v", (ROWS, 2 * WIDE), F32)],
        [VMEM((ROWS, GROUP_COLS), BF16), VMEM((ROWS, GROUP_COLS), BF16), VMEM((ROWS, FULL), BF16), dma((GROUPS,))],
    )(start, delta, bits, q, g, kv, kv2, kv1, ds2, ds1, near)
    key_gradient, value_gradient = call(sum_kernel, "sum", 1 << 20, "vvv", [narrow, narrow])(
        own, back2, back1
    )
    return query_grad, key_gradient, value_gradient


def solution(mesh):
    tokens = P(("ctx", "head"), None)
    return jax.shard_map(
        on_device,
        mesh=mesh,
        in_specs=(tokens,) * 5 + (P(),),
        out_specs=(tokens,) * 3,
        check_vma=False,
    )
```

```python
import jax
import jax.numpy as jnp
from jax import lax
from jax.experimental import pallas as pl
from jax.experimental.pallas import tpu as pltpu
from jax.sharding import PartitionSpec as P

HEADS = 32
GROUPS = 4
PER_GROUP = HEADS // GROUPS
PAIRS = PER_GROUP // 2
DIM = 128
ROWS = 128
WIDE = GROUPS * DIM
FULL = HEADS * DIM
GROUP_COLS = PER_GROUP * DIM
CHUNK = 128
SCALE = DIM ** (-0.5)
LOG2E = 1.4426950408889634
TO_BITS = SCALE * LOG2E
FILL = -1e30
VMEM = pltpu.VMEM
F32 = jnp.float32
BF16 = jnp.bfloat16
NT = (((1,), (1,)), ((), ()))
NN = (((1,), (0,)), ((), ()))


def dot(a, b, dims):
    return lax.dot_general(a, b, dims, preferred_element_type=F32)


def span(start, size):
    if isinstance(start, int):
        return pl.ds(start, size)
    return pl.ds(pl.multiple_of(start, DIM), size)


def stacked(ref, first, count):
    return jnp.concatenate([ref[:, span(first + i * DIM, DIM)] for i in range(count)], axis=0)


def pack_kernel(k_ref, v_ref, out_ref, sems):
    first = pltpu.make_async_copy(k_ref, out_ref.at[:, pl.ds(0, WIDE)], sems.at[0])
    second = pltpu.make_async_copy(v_ref, out_ref.at[:, pl.ds(WIDE, WIDE)], sems.at[1])
    first.start()
    second.start()
    first.wait()
    second.wait()


def local_kernel(
    pos_ref, len_hbm, q_hbm, g_hbm, o_hbm, kv_ref,
    q_ref, g_ref, start_ref, delta_ref, bits_ref, sum_ref,
    len_ref, o_ref, sems, len_sem,
):
    def copies(g):
        cols = span(g * GROUP_COLS, GROUP_COLS)
        return [
            pltpu.make_async_copy(src.at[:, cols], dst.at[:, cols], sems.at[i, g])
            for i, (src, dst) in enumerate(((q_hbm, q_ref), (g_hbm, g_ref), (o_hbm, o_ref)))
        ]

    len_copy = pltpu.make_async_copy(len_hbm, len_ref, len_sem)
    len_copy.start()
    for g in range(GROUPS):
        for copy in copies(g):
            copy.start()
    len_copy.wait()
    base = pos_ref[0]
    count = len_ref.shape[1]
    lengths = len_ref[...]
    high = lax.shift_right_logical(lengths, 4)
    low = lengths - high * 16
    both = jnp.concatenate(
        [jnp.broadcast_to(high, (8, count)), jnp.broadcast_to(low, (8, count))], axis=0
    ).astype(F32).astype(BF16)
    row = lax.broadcasted_iota(jnp.int32, (count, count), 0)
    col = lax.broadcasted_iota(jnp.int32, (count, count), 1)
    lower = jnp.where(col <= row, 1.0, 0.0).astype(BF16)
    sums = dot(lower, both, NT)
    ends = sums[:, 0:1] * 16.0 + sums[:, 8:9]
    tokens = (base + lax.broadcasted_iota(jnp.int32, (count, ROWS), 1)).astype(F32)
    starts = jnp.max(jnp.where(ends <= tokens, ends, 0.0), axis=0, keepdims=True)
    starts = starts - base.astype(F32)
    starts = jnp.concatenate([starts, starts], axis=1)
    start_ref[...] = jnp.broadcast_to(starts, (8, 2 * ROWS))
    key_at = lax.broadcasted_iota(jnp.int32, (ROWS, 2 * ROWS), 0)
    query_at = lax.broadcasted_iota(jnp.int32, (ROWS, 2 * ROWS), 1) & (ROWS - 1)
    seen = (key_at <= query_at) & (key_at.astype(F32) >= starts)

    def group(g, carry):
        for copy in copies(g):
            copy.wait()
        keys = kv_ref[:, span(g * DIM, DIM)]
        for p in range(PAIRS):
            pair = g * PAIRS + p
            first = pair * 2 * DIM
            deltas = []
            for h in range(2):
                cols = span(first + h * DIM, DIM)
                prod = g_ref[:, cols].astype(F32) * o_ref[:, cols].astype(F32)
                deltas.append(jnp.sum(prod.T, axis=0, keepdims=True))
            delta = jnp.concatenate(deltas, axis=1)
            here = pl.ds(p * 2 * DIM, 2 * DIM)
            delta_ref[pl.ds(g, 1), here] = delta.astype(BF16).astype(F32)
            scores = dot(keys, stacked(q_ref, first, 2), NT)
            scores = jnp.where(seen, scores, FILL)
            top = jnp.max(scores, axis=0, keepdims=True)
            bits = top * TO_BITS
            bits_ref[pl.ds(g, 1), here] = bits
            sum_ref[pl.ds(g, 1), here] = jnp.sum(
                jnp.exp2(scores * TO_BITS - bits), axis=0, keepdims=True
            )
        return carry

    for g in range(GROUPS):
        group(g, 0)


def pair_cols(p):
    return pl.ds(p * 2 * DIM, 2 * DIM)


def pre_kernel(
    start_ref, delta_ref, own_bits_ref, own_sum_ref, q_ref, g_ref, kv2_ref,
    exps_ref, grads_ref, bits_ref, sum_ref,
    bias_ref, score_ref,
):
    key_at = lax.broadcasted_iota(jnp.int32, (ROWS, 2 * ROWS), 0).astype(F32) - 2.0 * ROWS
    bias_ref[...] = jnp.where(key_at >= start_ref[0:1, :], 0.0, FILL)
    tops = {}

    def scores(g):
        keys = kv2_ref[:, span(g * DIM, DIM)]
        values = kv2_ref[:, span(WIDE + g * DIM, DIM)]
        for p in range(PAIRS):
            first = g * GROUP_COLS + p * 2 * DIM
            cols = span(first, 2 * DIM)
            value = dot(keys, stacked(q_ref, first, 2), NT) + bias_ref[...]
            score_ref[:, cols] = value
            tops[g, p] = jnp.max(value, axis=0, keepdims=True)
            grads = dot(values, stacked(g_ref, first, 2), NT)
            grads_ref[:, cols] = grads - delta_ref[g:g + 1, pair_cols(p)]

    def probs(g):
        for p in range(PAIRS):
            cols = span(g * GROUP_COLS + p * 2 * DIM, 2 * DIM)
            here = pair_cols(p)
            own_bits = own_bits_ref[g:g + 1, here]
            bits = jnp.maximum(tops[g, p] * TO_BITS, own_bits)
            bits_ref[g:g + 1, here] = bits
            exps = jnp.exp2(score_ref[:, cols] * TO_BITS - bits)
            exps_ref[:, cols] = exps
            sum_ref[g:g + 1, here] = jnp.sum(exps, axis=0, keepdims=True) + own_sum_ref[
                g:g + 1, here
            ] * jnp.exp2(own_bits - bits)

    scores(0)
    for g in range(GROUPS):
        if g + 1 < GROUPS:
            scores(g + 1)
        probs(g)


def mid_kernel(
    start_ref, far_bits_ref, far_sum_ref, exps_ref, grads_ref, q_ref, g_ref, kv1_ref,
    out_ref, ds2_ref, p1_ref, bits_ref,
    bias_ref, score_ref, p2_ref,
):
    key_at = lax.broadcasted_iota(jnp.int32, (ROWS, 2 * ROWS), 0).astype(F32) - 1.0 * ROWS
    bias_ref[...] = jnp.where(key_at >= start_ref[0:1, :], 0.0, FILL)
    tops = {}

    def scores(g):
        keys = kv1_ref[:, span(g * DIM, DIM)]
        for p in range(PAIRS):
            first = g * GROUP_COLS + p * 2 * DIM
            value = dot(keys, stacked(q_ref, first, 2), NT) + bias_ref[...]
            score_ref[:, span(first, 2 * DIM)] = value
            tops[g, p] = jnp.max(value, axis=0, keepdims=True)

    def probs(g):
        for p in range(PAIRS):
            first = g * GROUP_COLS + p * 2 * DIM
            cols = span(first, 2 * DIM)
            here = pair_cols(p)
            far_bits = far_bits_ref[g:g + 1, here]
            bits = jnp.maximum(tops[g, p] * TO_BITS, far_bits)
            total = jnp.zeros((CHUNK, 2 * DIM), F32)
            for r in range(0, ROWS, CHUNK):
                exps = jnp.exp2(score_ref[r:r + CHUNK, cols] * TO_BITS - bits)
                score_ref[r:r + CHUNK, cols] = exps
                total = total + exps
            scale = jnp.exp2(far_bits - bits)
            denom = jnp.sum(total, axis=0, keepdims=True) + far_sum_ref[g:g + 1, here] * scale
            inverse = 1.0 / denom
            weight = scale * inverse
            bits_ref[g:g + 1, here] = bits + jnp.log2(denom)
            for r in range(0, ROWS, CHUNK):
                value = exps_ref[r:r + CHUNK, cols] * weight
                p2_ref[r:r + CHUNK, cols] = value.astype(BF16)
                ds2_ref[r:r + CHUNK, cols] = (value * grads_ref[r:r + CHUNK, cols]).astype(BF16)
                p1_ref[r:r + CHUNK, cols] = (score_ref[r:r + CHUNK, cols] * inverse).astype(BF16)

    def sums(g):
        head0 = g * GROUP_COLS
        group_span = span(head0, GROUP_COLS)
        dk = dot(ds2_ref[:, group_span], stacked(q_ref, head0, PER_GROUP), NN)
        dv = dot(p2_ref[:, group_span], stacked(g_ref, head0, PER_GROUP), NN)
        out_ref[:, span(g * DIM, DIM)] = (dk * SCALE).astype(BF16)
        out_ref[:, span(WIDE + g * DIM, DIM)] = dv.astype(BF16)

    scores(0)
    for g in range(GROUPS):
        if g + 1 < GROUPS:
            scores(g + 1)
        probs(g)
        sums(g)


def near_kernel(delta_ref, p1_ref, q_ref, g_ref, kv1_ref, after_ref, out_ref, ds1_ref):
    def scores(g):
        values = kv1_ref[:, span(WIDE + g * DIM, DIM)]
        for p in range(PAIRS):
            first = g * GROUP_COLS + p * 2 * DIM
            cols = span(first, 2 * DIM)
            grads = dot(values, stacked(g_ref, first, 2), NT)
            probs = p1_ref[:, cols].astype(F32)
            ds1_ref[:, cols] = (probs * (grads - delta_ref[g:g + 1, pair_cols(p)])).astype(BF16)

    def sums(g):
        head0 = g * GROUP_COLS
        group_span = span(head0, GROUP_COLS)
        dv = dot(p1_ref[:, group_span], stacked(g_ref, head0, PER_GROUP), NN)
        dk = dot(ds1_ref[:, group_span], stacked(q_ref, head0, PER_GROUP), NN)
        out_ref[:, span(g * DIM, DIM)] = (dk * SCALE).astype(BF16)
        out_ref[:, span(WIDE + g * DIM, DIM)] = dv.astype(BF16)

    scores(0)
    for g in range(GROUPS):
        if g + 1 < GROUPS:
            scores(g + 1)
        sums(g)


def own_kernel(
    start_ref, delta_ref, bits_ref, q_ref, g_ref, kv_ref, kv2_ref, kv1_ref, ds2_ref, ds1_ref, after_ref,
    dq_hbm, out_ref,
    ds_ref, p_ref, dq_ref, sems,
):
    key_at = lax.broadcasted_iota(jnp.int32, (ROWS, 2 * ROWS), 0)
    query_at = lax.broadcasted_iota(jnp.int32, (ROWS, 2 * ROWS), 1) & (ROWS - 1)
    seen = (key_at <= query_at) & (key_at.astype(F32) >= start_ref[0:1, :])

    def copy(g):
        cols = span(g * GROUP_COLS, GROUP_COLS)
        return pltpu.make_async_copy(dq_ref.at[:, cols], dq_hbm.at[:, cols], sems.at[g])

    def group(g, carry):
        gcols = span(g * DIM, DIM)
        vcols = span(WIDE + g * DIM, DIM)
        keys = kv_ref[:, gcols]
        values = kv_ref[:, vcols]
        turned = jnp.concatenate([kv2_ref[:, gcols].T, kv1_ref[:, gcols].T, keys.T], axis=1)
        for p in range(PAIRS):
            pair = g * PAIRS + p
            first = pair * 2 * DIM
            cols = span(first, 2 * DIM)
            here = pl.ds(p * 2 * DIM, 2 * DIM)
            scores = dot(keys, stacked(q_ref, first, 2), NT)
            probs = jnp.exp2(
                jnp.where(seen, scores * TO_BITS - bits_ref[pl.ds(g, 1), pair_cols(p)], FILL)
            )
            grads = dot(values, stacked(g_ref, first, 2), NT)
            low = (probs * (grads - delta_ref[pl.ds(g, 1), pair_cols(p)])).astype(BF16)
            ds_ref[:, here] = low
            p_ref[:, here] = probs.astype(BF16)
            score_grads = jnp.concatenate([ds2_ref[:, cols], ds1_ref[:, cols], low], axis=0)
            turned_grad = dot(turned, score_grads, NN) * SCALE
            for h in range(2):
                dq_ref[:, span(first + h * DIM, DIM)] = (
                    turned_grad[:, h * DIM:(h + 1) * DIM].T.astype(BF16)
                )
        copy(g).start()
        head0 = g * GROUP_COLS
        dk = dot(ds_ref[...], stacked(q_ref, head0, PER_GROUP), NN)
        dv = dot(p_ref[...], stacked(g_ref, head0, PER_GROUP), NN)
        out_ref[:, gcols] = dk * SCALE
        out_ref[:, vcols] = dv
        return carry

    for g in range(GROUPS):
        group(g, 0)
    for g in range(GROUPS):
        copy(g).wait()


def sum_kernel(own_ref, far_ref, near_ref, dk_hbm, dv_hbm, total_ref, sems):
    copies = []
    for part, ref in ((0, dk_hbm), (1, dv_hbm)):
        cols = pl.ds(part * WIDE, WIDE)
        total = own_ref[:, cols] + far_ref[:, cols].astype(F32) + near_ref[:, cols].astype(F32)
        total_ref[:, cols] = total.astype(BF16)
        copy = pltpu.make_async_copy(total_ref.at[:, cols], ref, sems.at[part])
        copy.start()
        copies.append(copy)
    for copy in copies:
        copy.wait()


def call(body, name, flops, ins, outs, scratch=()):
    spaces = {"s": pltpu.SMEM, "v": VMEM, "a": pl.ANY, "h": pltpu.HBM}
    return pl.pallas_call(
        body,
        name=name,
        in_specs=[pl.BlockSpec(memory_space=spaces[space]) for space in ins],
        out_specs=[pl.BlockSpec(memory_space=spaces[space]) for space, _, _ in outs],
        out_shape=[jax.ShapeDtypeStruct(shape, dtype) for _, shape, dtype in outs],
        scratch_shapes=list(scratch),
        cost_estimate=pl.CostEstimate(flops=flops, transcendentals=0, bytes_accessed=1 << 20),
        compiler_params=pltpu.CompilerParams(vmem_limit_bytes=12 << 20),
    )


def on_device(queries, keys, values, attn_out, output_gradient, doc_lengths):
    contexts = lax.axis_size("ctx")
    halves = lax.axis_size("head")
    blocks = contexts * halves
    count = doc_lengths.shape[0]

    def shifted(array, by):
        place = lambda i: (i % halves) * contexts + i // halves
        pairs = [(place(i), place(i + by)) for i in range(blocks) if 0 <= i + by < blocks]
        return lax.ppermute(array, ("head", "ctx"), pairs)

    keys, values, queries, attn_out, output_gradient, lengths = (
        pltpu.with_memory_space_constraint(array, pltpu.HBM)
        for array in (keys, values, queries, attn_out, output_gradient, doc_lengths.reshape(1, -1))
    )
    base = ((lax.axis_index("ctx") * halves + lax.axis_index("head")) * ROWS).reshape(1)
    stat = ("v", (8, GROUP_COLS), F32)
    rows = ("v", (8, 2 * ROWS), F32)
    both = ("v", (ROWS, 2 * WIDE), BF16)
    full = ("v", (ROWS, FULL), BF16)
    narrow = ("h", (ROWS, WIDE), BF16)
    dma = pltpu.SemaphoreType.DMA
    (kv,) = call(pack_kernel, "pack", 1 << 20, "hh", [both], [dma((2,))])(keys, values)
    kv2 = shifted(kv, 2)
    kv1 = shifted(kv, 1)
    q, g, start, delta, own_bits, own_sum = call(
        local_kernel, "local", 1 << 30, "shhhhv", [full, full, rows, stat, stat, stat],
        [VMEM((1, count), jnp.int32), VMEM((ROWS, FULL), BF16), dma((3, GROUPS)), dma],
    )(base, lengths, queries, output_gradient, attn_out, kv)
    exact = ("v", (ROWS, FULL), F32)
    bias = VMEM((ROWS, 2 * ROWS), F32)
    exact_scratch = VMEM((ROWS, FULL), F32)
    exps, grads, far_bits, far_sum = call(
        pre_kernel, "pre", 1 << 30, "v" * 7, [exact, exact, stat, stat], [bias, exact_scratch]
    )(start, delta, own_bits, own_sum, q, g, kv2)
    far, ds2, p1, bits = call(
        mid_kernel, "mid", 1 << 30, "v" * 8, [both, full, full, stat],
        [bias, exact_scratch, VMEM((ROWS, FULL), BF16)],
    )(start, far_bits, far_sum, exps, grads, q, g, kv1)
    back2 = shifted(far, -2)
    near, ds1 = call(near_kernel, "near", 1 << 30, "v" * 5 + "a", [both, full])(
        delta, p1, q, g, kv1, far
    )
    back1 = shifted(near, -1)
    query_grad, own = call(
        own_kernel, "own", 4 << 30, "v" * 10 + "a",
        [("h", (ROWS, FULL), BF16), ("v", (ROWS, 2 * WIDE), F32)],
        [VMEM((ROWS, GROUP_COLS), BF16), VMEM((ROWS, GROUP_COLS), BF16), VMEM((ROWS, FULL), BF16), dma((GROUPS,))],
    )(start, delta, bits, q, g, kv, kv2, kv1, ds2, ds1, near)
    key_gradient, value_gradient = call(sum_kernel, "sum", 1 << 20, "vvv", [narrow, narrow], [VMEM((ROWS, 2 * WIDE), BF16), dma((2,))])(
        own, back2, back1
    )
    return query_grad, key_gradient, value_gradient


def solution(mesh):
    tokens = P(("ctx", "head"), None)
    return jax.shard_map(
        on_device,
        mesh=mesh,
        in_specs=(tokens,) * 5 + (P(),),
        out_specs=(tokens,) * 3,
        check_vma=False,
    )
```
